32 devices in a mesh: tm: 4 (over y, x), lat: 8 (over z, core).
Axes of the slice: x: 2, y: 2, z: 4, core: 2. Of those that a mesh axis runs over, the one named last changes fastest.
Arguments:
- sketch: bfloat16 [256, 3, 64, 1024], P('tm', None, 'lat'), may hold values from -6 to 6
- test_sketch: bfloat16 [256, 3, 64, 1024], P('tm', None, 'lat'), may hold values from -6 to 6
- checkpoints: bfloat16 [16, 3, 64, 1024], P('tm', None, 'lat'), may hold values from -2.5 to 2.5
- checkpoint_step: int32 [4], P('tm'), may hold values from 0 to 3
- station_row: int32 [4, 1024], P('tm', 'lat'), may hold values from 0 to 63, as said below
- station_column: int32 [4, 1024], P('tm', 'lat'), may hold values from 0 to 1023
- station_value: float32 [4, 1024], P('tm', 'lat'), may hold values from -6 to 6
Outputs:
- increment: float32 [4, 3, 64, 1024], P('tm', None, 'lat')
- reduced_adjoint: float32 [4, 64], P('tm')
- total_cost: float32 [], replicated
The draws below stay inside these ranges and needn't reach their ends.
Inputs may be any that keep to these rules, and one draw needn't show every extreme that they name: `station_row`: in each group's list, entries 128 * j to 128 * (j + 1) - 1 lie in latitude rows 8 * j to 8 * (j + 1) - 1.
All inputs are finite; a program needn't handle non-finite values.
Results may differ from the reference program's by a relative error of at most 0.0003.
Values may be sent and summed in bfloat16 or wider, within the bound.
A program may use at most 128 MiB of HBM per device.

```python
import math
import jax
import jax.numpy as jnp
from jax import lax

K = 64
ROWS = 8
NLON = 1024
STEPS = 4
NCK = 4
OBS_DEV = 128
NLAT = 64
NOBS = 1024
N_TM = 4


def draw_station_row(key, part):
    band = jnp.arange(NOBS, dtype=jnp.int32) // OBS_DEV
    offset = jax.random.randint(key, (N_TM, NOBS), 0, ROWS, dtype=jnp.int32)
    return band[None, :] * ROWS + offset


def plant(values, key, least, top_value):
    longest = values.shape.index(max(values.shape))
    spots = []
    for shift in (0, 1):
        where = [jax.random.randint(jax.random.fold_in(key, axis), (), 0, length) for axis, length in enumerate(values.shape)]
        where[longest] = (where[longest] + shift) % values.shape[longest]
        spots.append(tuple(where))
    return values.at[spots[0]].set(least).at[spots[1]].set(top_value)


def block_levels(own_key, shape, cuts, low, top_value):
    def one(position, parts):
        draws = jax.random.uniform(jax.random.fold_in(jax.random.fold_in(own_key, 6), position), (parts,), jnp.float32, low / len(cuts), top_value / len(cuts))
        return jnp.repeat(jnp.exp(draws), shape[position] // parts).reshape((-1,) + (1,) * (len(shape) - position - 1))

    factor_of = one(*cuts[0])
    for cut in cuts[1:]:
        factor_of = factor_of * one(*cut)
    return factor_of


def gaussian(key, extent, spread, reach, split=(), kind=jnp.bfloat16):
    loudness = block_levels(key, extent, split, -0.22, 0.18) if split else 1.0
    drawn = jax.random.normal(key, extent, jnp.float32) * spread * loudness
    return jnp.minimum(jnp.maximum(drawn, -reach), reach).astype(kind)


def setup_inputs(seed: int = 0) -> dict:
    arg_keys = jax.random.split(jax.random.key(seed), 8)
    return {
        "sketch": gaussian(arg_keys[0], (N_TM * K, 3, NLAT, NLON), 1.0, 6.0, ((0, 4), (2, 8))),
        "test_sketch": gaussian(arg_keys[1], (N_TM * K, 3, NLAT, NLON), 1.0, 6.0, ((0, 4), (2, 8))),
        "checkpoints": gaussian(arg_keys[2], (N_TM * NCK, 3, NLAT, NLON), 1.0, 2.5, ((0, 4), (2, 8))),
        "checkpoint_step": plant(jax.random.randint(arg_keys[3], (N_TM,), 0, NCK), jax.random.fold_in(arg_keys[3], 1), 0, NCK - 1).astype(jnp.int32),
        "station_row": draw_station_row(jax.random.fold_in(arg_keys[7], 71), 0),
        "station_column": plant(jax.random.randint(arg_keys[5], (N_TM, NOBS), 0, NLON), jax.random.fold_in(arg_keys[5], 1), 0, NLON - 1).astype(jnp.int32),
        "station_value": gaussian(arg_keys[6], (N_TM, NOBS), 1.0, 6.0, ((0, 4), (1, 8)), jnp.float32),
    }


wave_coef = 0.5
flow_coef = 0.4
coriolis_coef = 0.5
map_scale = 0.5

def coefficients(base_rows, first_row, total_rows):
    values = base_rows.astype(jnp.float32)
    depth = 1.0 + 0.25 * values[0]
    east_flow = 0.4 * values[1]
    north_flow = 0.4 * values[2]
    latitude = (first_row + jnp.arange(values.shape[1], dtype=jnp.int32)).astype(jnp.float32)
    coriolis = coriolis_coef * (2.0 * (latitude + 0.5) / total_rows - 1.0)
    return (depth, east_flow, north_flow, coriolis[:, None])

def advance(padded, depth, east_flow, north_flow, coriolis):
    height = padded[:, 0]
    eastward = padded[:, 1]
    northward = padded[:, 2]

    def along_lon(field):
        middle = field[:, 1:-1]
        return 0.5 * (jnp.roll(middle, -1, -1) - jnp.roll(middle, 1, -1))

    def along_lat(field):
        return 0.5 * (field[:, 2:] - field[:, :-2])
    centre_height = height[:, 1:-1]
    centre_east = eastward[:, 1:-1]
    centre_north = northward[:, 1:-1]
    new_east = centre_east + wave_coef * (coriolis * centre_north - along_lon(height)) - flow_coef * (east_flow * along_lon(eastward) + north_flow * along_lat(eastward))
    new_north = centre_north + wave_coef * (-coriolis * centre_east - along_lat(height)) - flow_coef * (east_flow * along_lon(northward) + north_flow * along_lat(northward))
    new_height = centre_height - wave_coef * depth * (along_lon(eastward) + along_lat(northward)) - flow_coef * (east_flow * along_lon(height) + north_flow * along_lat(height))
    return jnp.stack([new_height, new_east, new_north], 1)

def one_group(inputs):
    basis, tests, stored, chosen, rows, columns, values = inputs
    base = lax.dynamic_index_in_dim(stored, chosen, 0, keepdims=False)
    depth, east_flow, north_flow, coriolis = coefficients(base, 0, NLAT)
    state = basis.astype(jnp.float32)
    for step_index in range(STEPS):
        padded = jnp.pad(state, ((0, 0), (0, 0), (1, 1), (0, 0)))
        state = advance(padded, depth, east_flow, north_flow, coriolis)
    propagator = lax.dot_general(tests.reshape(K, -1).astype(jnp.float32), state.reshape(K, -1), (((1,), (1,)), ((), ())), precision=lax.Precision.HIGHEST, preferred_element_type=jnp.float32) * (map_scale / math.sqrt(K * 3 * NLAT * NLON))
    flat = (rows * NLON + columns).astype(jnp.int32)
    heights = basis[:, 0].reshape(K, -1)
    sampled = jnp.take(heights, flat, axis=1).astype(jnp.float32)
    innovation = jnp.take(base[0].reshape(-1), flat).astype(jnp.float32) - values
    weight = 1.0 + 2.0 * rows.astype(jnp.float32) / NLAT
    forcing = jnp.dot(sampled, weight * innovation, precision=lax.Precision.HIGHEST) / (2.0 * math.sqrt(NOBS))
    cost = jnp.sum(weight * innovation * innovation) / (2.0 * N_TM * NOBS)
    return (state, propagator, forcing, cost)

def reference(sketch, test_sketch, checkpoints, checkpoint_step, station_row, station_column, station_value):
    inputs = (sketch.reshape(N_TM, K, 3, NLAT, NLON), test_sketch.reshape(N_TM, K, 3, NLAT, NLON), checkpoints.reshape(N_TM, NCK, 3, NLAT, NLON), checkpoint_step, station_row, station_column, station_value)
    states, propagators, forcings, costs = lax.map(one_group, inputs)
    following = jnp.zeros((K,), jnp.float32)
    adjoints = [None] * N_TM
    for group in reversed(range(N_TM)):
        adjoint = jnp.dot(propagators[group].T, following, precision=lax.Precision.HIGHEST) + forcings[group]
        adjoints[group] = adjoint
        following = adjoint
    adjoint_stack = jnp.stack(adjoints)
    increment = jnp.einsum('gk,gkfrc->gfrc', adjoint_stack, states, precision=lax.Precision.HIGHEST) / math.sqrt(K)
    return (increment, adjoint_stack, jnp.sum(costs))
```

```python
import functools
import math

import jax
import jax.numpy as jnp
from jax import lax
from jax.experimental import pallas as pl
from jax.experimental.pallas import tpu as pltpu
from jax.sharding import PartitionSpec as P

STEPS = 4
LANES = 128

wave_coef = 0.5
flow_coef = 0.4
coriolis_coef = 0.5
map_scale = 0.5

MESH = pl.DeviceIdType.MESH


def dlon(field):
    count = field.shape[1]
    return pltpu.roll(field, count - 1, 1) - pltpu.roll(field, 1, 1)


def dlat(field):
    count = field.shape[0]
    return pltpu.roll(field, count - 1, 0) - pltpu.roll(field, 1, 0)


def advance(state, coefs):
    height, east, north = state
    depth, east_flow, north_flow, turn, keep = coefs
    half = 0.5 * wave_coef
    dx_east, dy_north = dlon(east), dlat(north)
    dx_height, dy_height = dlon(height), dlat(height)
    new_east = (
        east + turn * north - half * dx_height - (east_flow * dx_east + north_flow * dlat(east))
    )
    new_north = (
        north - turn * east - half * dy_height - (east_flow * dlon(north) + north_flow * dy_north)
    )
    new_height = (
        height - depth * (dx_east + dy_north) - (east_flow * dx_height + north_flow * dy_height)
    )
    return new_height * keep, new_east * keep, new_north * keep


def advance_adjoint(state, coefs):
    height, east, north = state
    depth, east_flow, north_flow, turn, keep = coefs
    half = 0.5 * wave_coef
    deep = depth * height
    new_height = height + dlon(half * east + east_flow * height) + dlat(
        half * north + north_flow * height
    )
    new_east = east - turn * north + dlon(deep + east_flow * east) + dlat(north_flow * east)
    new_north = north + turn * east + dlon(east_flow * north) + dlat(deep + north_flow * north)
    return new_height * keep, new_east * keep, new_north * keep


def kernel(
    groups,
    bands,
    sketch_hbm,
    test_hbm,
    stored,
    chosen,
    station_row,
    station_column,
    station_value,
    increment,
    adjoint,
    total_cost,
    sketch,
    test,
    coef_ext,
    ext,
    forced,
    folded,
    spread,
    base_send,
    base_recv,
    field_send,
    field_recv,
    last_send,
    last_recv,
    message,
    later_in,
    own_in,
    cost_out,
    cost_in,
    cost_group_out,
    cost_group_in,
    load_sem,
    base_ss,
    base_rs,
    field_ss,
    field_rs,
    last_ss,
    last_rs,
    later_ss,
    later_rs,
    own_ss,
    own_rs,
    cost_ss,
    cost_rs,
    cost_group_ss,
    cost_group_rs,
):
    rank, fields, rows, columns = sketch.shape
    halo = STEPS
    group = lax.axis_index("tm")
    band = lax.axis_index("lat")
    total_rows = rows * bands
    observed = station_row.shape[1] * bands
    tiles = columns // LANES

    load_sketch = pltpu.make_async_copy(sketch_hbm, sketch, load_sem.at[0])
    load_test = pltpu.make_async_copy(test_hbm, test, load_sem.at[1])
    load_sketch.start()
    load_test.start()

    barrier = pltpu.get_barrier_semaphore()
    devices = groups * bands
    me = group * bands + band

    def greet(offset, carry):
        other = lax.rem(me + offset, devices)
        pl.semaphore_signal(
            barrier,
            inc=1,
            device_id={"tm": other // bands, "lat": lax.rem(other, bands)},
            device_id_type=MESH,
        )
        return carry

    lax.fori_loop(1, devices, greet, 0)

    def remote(source, target, send_sem, recv_sem, where):
        return pltpu.make_async_remote_copy(
            src_ref=source,
            dst_ref=target,
            send_sem=send_sem,
            recv_sem=recv_sem,
            device_id=where,
            device_id_type=MESH,
        )

    def halo_copies(send, recv, ss, rs):
        down = remote(send.at[0], recv.at[1], ss.at[0], rs.at[1], {"lat": jnp.maximum(band - 1, 0)})
        up = remote(
            send.at[1], recv.at[0], ss.at[1], rs.at[0], {"lat": jnp.minimum(band + 1, bands - 1)}
        )
        return down, up

    def halo_start(send, recv, ss, rs):
        down, up = halo_copies(send, recv, ss, rs)

        @pl.when(band > 0)
        def _():
            down.start()

        @pl.when(band == 0)
        def _():
            recv[0] = jnp.zeros(recv.shape[1:], recv.dtype)

        @pl.when(band < bands - 1)
        def _():
            up.start()

        @pl.when(band == bands - 1)
        def _():
            recv[1] = jnp.zeros(recv.shape[1:], recv.dtype)

    def halo_wait(send, recv, ss, rs):
        down, up = halo_copies(send, recv, ss, rs)

        @pl.when(band > 0)
        def _():
            up.wait_recv()

        @pl.when(band < bands - 1)
        def _():
            down.wait_recv()

    def halo_drain(send, recv, ss, rs):
        down, up = halo_copies(send, recv, ss, rs)

        @pl.when(band > 0)
        def _():
            down.wait_send()

        @pl.when(band < bands - 1)
        def _():
            up.wait_send()

    base_half = stored[chosen[0]]
    base = base_half.astype(jnp.float32)
    base_send[0] = base[:, :halo]
    base_send[1] = base[:, rows - halo :]

    cells = lax.broadcasted_iota(jnp.int32, (columns, station_column.shape[1]), 0)
    at_column = cells == station_column[...]
    local_row = station_row[...] - band * rows
    at_row = (
        lax.broadcasted_iota(jnp.int32, (rows, station_row.shape[1]), 0) == local_row
    )
    one_hot = at_column.astype(jnp.float32)
    by_row = jnp.dot(
        base_half[0],
        one_hot.astype(jnp.bfloat16),
        preferred_element_type=jnp.float32,
    )
    seen = jnp.sum(jnp.where(at_row, by_row, 0.0), axis=0, keepdims=True)
    innovation = seen - station_value[...]
    weight = 1.0 + 2.0 * station_row[...].astype(jnp.float32) / total_rows
    weighted = weight * innovation
    cost = jnp.sum(weighted * innovation, axis=1, keepdims=True) / (2.0 * groups * observed)
    cost_row = jnp.broadcast_to(cost, (1, LANES))
    cost_out[...] = cost_row
    source = jnp.where(at_row, weighted / (2.0 * math.sqrt(observed)), 0.0)
    forced[0] = lax.dot_general(
        source,
        one_hot,
        (((1,), (1,)), ((), ())),
        precision=lax.Precision.HIGHEST,
        preferred_element_type=jnp.float32,
    )
    for field in range(1, fields):
        forced[field] = jnp.zeros((rows, columns), jnp.float32)

    pl.semaphore_wait(barrier, devices - 1)

    halo_start(base_send, base_recv, base_ss, base_rs)

    def cost_copy(offset):
        other = lax.rem(band + offset, bands)
        return remote(
            cost_out, cost_in.at[band], cost_ss.at[offset], cost_rs.at[band], {"lat": other}
        )

    def cost_arrival(offset):
        other = lax.rem(band + offset, bands)
        return remote(
            cost_out, cost_in.at[other], cost_ss.at[offset], cost_rs.at[other], {"lat": other}
        )

    def each(count, first, action):
        def step(index, carry):
            action(index)
            return carry

        lax.fori_loop(first, count, step, 0)

    each(bands, 1, lambda offset: cost_copy(offset).start())
    cost_in[band] = cost_row

    halo_wait(base_send, base_recv, base_ss, base_rs)
    for field in range(fields):
        coef_ext[field, pl.ds(0, halo)] = base_recv[0, field]
        coef_ext[field, pl.ds(halo, rows)] = base[field]
        coef_ext[field, pl.ds(halo + rows, halo)] = base_recv[1, field]
    coef_ext[0] = 0.5 * wave_coef * (1.0 + 0.25 * coef_ext[0])
    coef_ext[1] = 0.5 * flow_coef * 0.4 * coef_ext[1]
    coef_ext[2] = 0.5 * flow_coef * 0.4 * coef_ext[2]
    span = rows + 2 * halo

    def coefs():
        where = band * rows - halo + lax.broadcasted_iota(jnp.int32, (span, columns), 0)
        latitude = where.astype(jnp.float32)
        turn = wave_coef * coriolis_coef * (2.0 * (latitude + 0.5) / total_rows - 1.0)
        keep = jnp.where((where >= 0) & (where < total_rows), 1.0, 0.0)
        return coef_ext[0], coef_ext[1], coef_ext[2], turn, keep

    def marched(step_of, send, recv, ss, rs):
        halo_start(send, recv, ss, rs)
        halo_wait(send, recv, ss, rs)
        for field in range(fields):
            ext[field, pl.ds(0, halo)] = recv[0, field]
            ext[field, pl.ds(halo + rows, halo)] = recv[1, field]

        def one(index, carry):
            result = step_of((ext[0], ext[1], ext[2]), coefs())
            for field in range(fields):
                ext[field] = result[field]
            return carry

        lax.fori_loop(0, STEPS, one, 0)

    eye = lax.broadcasted_iota(jnp.int32, (rank, LANES), 0) == lax.broadcasted_iota(
        jnp.int32, (rank, LANES), 1
    )

    def spread_row(row):
        column = jnp.sum(jnp.where(eye, row, 0.0), axis=1, keepdims=True)
        spread[...] = jnp.broadcast_to(column, (rank, LANES))

    block = 4

    def combined(basis, send):
        for field in range(fields):

            def some(index, total):
                for inner in range(block):
                    k = index * block + inner
                    factor = jnp.broadcast_to(spread[pl.ds(k, 1), :], (rows, LANES))
                    total = total + basis[k, field].astype(jnp.float32) * jnp.concatenate(
                        [factor] * tiles, axis=1
                    )
                return total

            total = lax.fori_loop(
                0, rank // block, some, jnp.zeros((rows, columns), jnp.float32)
            )
            ext[field, pl.ds(halo, rows)] = total
            send[0, field] = total[:halo]
            send[1, field] = total[rows - halo :]

    load_sketch.wait()
    load_test.wait()

    @pl.when(group < groups - 1)
    def _():
        def arrive(offset):
            remote(
                message,
                later_in.at[offset],
                later_ss.at[offset],
                later_rs.at[offset],
                {"tm": group, "lat": offset},
            ).wait_recv()

        each(bands, 0, arrive)
        spread_row(jnp.sum(later_in[...], axis=0))
        combined(test, field_send)
        marched(advance_adjoint, field_send, field_recv, field_ss, field_rs)
        scale = map_scale / math.sqrt(rank * fields * total_rows * columns)
        for field in range(fields):
            forced[field] = forced[field] + scale * ext[field, pl.ds(halo, rows)]

    def fold(index, carry):
        for inner in range(block):
            k = index * block + inner
            product = sketch[k, 0].astype(jnp.float32) * forced[0]
            for field in range(1, fields):
                product = product + sketch[k, field].astype(jnp.float32) * forced[field]
            total = product[:, :LANES]
            for tile in range(1, tiles):
                total = total + product[:, tile * LANES : (tile + 1) * LANES]
            folded[k] = total
        return carry

    lax.fori_loop(0, rank // block, fold, 0)
    share = jnp.sum(jnp.sum(folded[...], axis=1), axis=1, keepdims=True)
    share_row = jnp.sum(jnp.where(eye, share, 0.0), axis=0, keepdims=True)
    message[...] = share_row

    def later_copy(offset):
        other = lax.rem(band + offset, bands)
        return remote(
            message,
            later_in.at[band],
            later_ss.at[offset],
            later_rs.at[band],
            {"tm": jnp.maximum(group - 1, 0), "lat": other},
        )

    @pl.when(group > 0)
    def _():
        each(bands, 0, lambda offset: later_copy(offset).start())

    def own_copy(offset):
        other = lax.rem(band + offset, bands)
        return remote(
            message, own_in.at[band], own_ss.at[offset], own_rs.at[band], {"lat": other}
        )

    def own_arrival(offset):
        other = lax.rem(band + offset, bands)
        return remote(
            message, own_in.at[other], own_ss.at[offset], own_rs.at[other], {"lat": other}
        )

    each(bands, 1, lambda offset: own_copy(offset).start())
    own_in[band] = share_row

    each(bands, 1, lambda offset: cost_arrival(offset).wait_recv())
    group_cost = jnp.sum(cost_in[...], axis=0)
    cost_group_out[...] = group_cost

    def cost_group_copy(offset):
        other = lax.rem(group + offset, groups)
        return remote(
            cost_group_out,
            cost_group_in.at[group],
            cost_group_ss.at[offset],
            cost_group_rs.at[group],
            {"tm": other},
        )

    def cost_group_arrival(offset):
        other = lax.rem(group + offset, groups)
        return remote(
            cost_group_out,
            cost_group_in.at[other],
            cost_group_ss.at[offset],
            cost_group_rs.at[other],
            {"tm": other},
        )

    each(groups, 1, lambda offset: cost_group_copy(offset).start())
    cost_group_in[group] = group_cost

    each(bands, 1, lambda offset: own_arrival(offset).wait_recv())
    adjoint_row = jnp.sum(own_in[...], axis=0)
    adjoint[...] = adjoint_row[:, :rank]
    spread_row(adjoint_row)
    combined(sketch, last_send)
    marched(advance, last_send, last_recv, last_ss, last_rs)
    for field in range(fields):
        increment[0, field] = ext[field, pl.ds(halo, rows)] / math.sqrt(rank)

    each(groups, 1, lambda offset: cost_group_arrival(offset).wait_recv())
    total_cost[...] = jnp.sum(cost_group_in[...], axis=0)[:, :1]

    halo_drain(base_send, base_recv, base_ss, base_rs)
    halo_drain(last_send, last_recv, last_ss, last_rs)
    each(bands, 1, lambda offset: cost_copy(offset).wait_send())
    each(bands, 1, lambda offset: own_copy(offset).wait_send())
    each(groups, 1, lambda offset: cost_group_copy(offset).wait_send())

    @pl.when(group < groups - 1)
    def _():
        halo_drain(field_send, field_recv, field_ss, field_rs)

    @pl.when(group > 0)
    def _():
        each(bands, 0, lambda offset: later_copy(offset).wait_send())


def body(
    groups,
    bands,
    sketch,
    test_sketch,
    checkpoints,
    checkpoint_step,
    station_row,
    station_column,
    station_value,
):
    rank, fields, rows, columns = sketch.shape
    span = rows + 2 * STEPS
    f32 = jnp.float32
    vmem = pl.BlockSpec(memory_space=pltpu.VMEM)
    edge = pltpu.VMEM((2, fields, STEPS, columns), f32)
    dma = pltpu.SemaphoreType.DMA
    increment, adjoint, cost = pl.pallas_call(
        functools.partial(kernel, groups, bands),
        out_shape=(
            jax.ShapeDtypeStruct((1, fields, rows, columns), f32),
            jax.ShapeDtypeStruct((1, rank), f32),
            jax.ShapeDtypeStruct((1, 1), f32),
        ),
        in_specs=[
            pl.BlockSpec(memory_space=pl.ANY),
            pl.BlockSpec(memory_space=pl.ANY),
            vmem,
            pl.BlockSpec(memory_space=pltpu.SMEM),
            vmem,
            vmem,
            vmem,
        ],
        out_specs=(vmem, vmem, vmem),
        scratch_shapes=[
            pltpu.VMEM(sketch.shape, sketch.dtype),
            pltpu.VMEM(test_sketch.shape, test_sketch.dtype),
            pltpu.VMEM((fields, span, columns), f32),
            pltpu.VMEM((fields, span, columns), f32),
            pltpu.VMEM((fields, rows, columns), f32),
            pltpu.VMEM((rank, rows, LANES), f32),
            pltpu.VMEM((rank, LANES), f32),
            edge,
            edge,
            edge,
            edge,
            edge,
            edge,
            pltpu.VMEM((1, LANES), f32),
            pltpu.VMEM((bands, 1, LANES), f32),
            pltpu.VMEM((bands, 1, LANES), f32),
            pltpu.VMEM((1, LANES), f32),
            pltpu.VMEM((bands, 1, LANES), f32),
            pltpu.VMEM((1, LANES), f32),
            pltpu.VMEM((groups, 1, LANES), f32),
            dma((2,)),
            dma((2,)),
            dma((2,)),
            dma((2,)),
            dma((2,)),
            dma((2,)),
            dma((2,)),
            dma((bands,)),
            dma((bands,)),
            dma((bands,)),
            dma((bands,)),
            dma((bands,)),
            dma((bands,)),
            dma((groups,)),
            dma((groups,)),
        ],
        compiler_params=pltpu.CompilerParams(
            collective_id=0,
            has_side_effects=True,
            vmem_limit_bytes=40 * 1024 * 1024,
        ),
    )(
        sketch,
        test_sketch,
        checkpoints,
        checkpoint_step,
        station_row,
        station_column,
        station_value,
    )
    return increment, adjoint, cost[0, 0]


def solution(mesh):
    placed = (
        P("tm", None, "lat", None),
        P("tm", None, "lat", None),
        P("tm", None, "lat", None),
        P("tm"),
        P("tm", "lat"),
        P("tm", "lat"),
        P("tm", "lat"),
    )
    return jax.shard_map(
        functools.partial(body, mesh.shape["tm"], mesh.shape["lat"]),
        mesh=mesh,
        in_specs=placed,
        out_specs=(P("tm", None, "lat", None), P("tm", None), P()),
        check_vma=False,
    )
```

```python
import functools
import math

import jax
import jax.numpy as jnp
from jax import lax
from jax.experimental import pallas as pl
from jax.experimental.pallas import tpu as pltpu
from jax.sharding import PartitionSpec as P

STEPS = 4
LANES = 128

wave_coef = 0.5
flow_coef = 0.4
coriolis_coef = 0.5
map_scale = 0.5

MESH = pl.DeviceIdType.MESH


def dlon(field):
    count = field.shape[1]
    return pltpu.roll(field, count - 1, 1) - pltpu.roll(field, 1, 1)


def dlat(field):
    count = field.shape[0]
    return pltpu.roll(field, count - 1, 0) - pltpu.roll(field, 1, 0)


def advance(state, coefs):
    height, east, north = state
    depth, east_flow, north_flow, turn, keep = coefs
    half = 0.5 * wave_coef
    dx_east, dy_north = dlon(east), dlat(north)
    dx_height, dy_height = dlon(height), dlat(height)
    new_east = (
        east + turn * north - half * dx_height - (east_flow * dx_east + north_flow * dlat(east))
    )
    new_north = (
        north - turn * east - half * dy_height - (east_flow * dlon(north) + north_flow * dy_north)
    )
    new_height = (
        height - depth * (dx_east + dy_north) - (east_flow * dx_height + north_flow * dy_height)
    )
    return new_height * keep, new_east * keep, new_north * keep


def advance_adjoint(state, coefs):
    height, east, north = state
    depth, east_flow, north_flow, turn, keep = coefs
    half = 0.5 * wave_coef
    deep = depth * height
    new_height = height + dlon(half * east + east_flow * height) + dlat(
        half * north + north_flow * height
    )
    new_east = east - turn * north + dlon(deep + east_flow * east) + dlat(north_flow * east)
    new_north = north + turn * east + dlon(east_flow * north) + dlat(deep + north_flow * north)
    return new_height * keep, new_east * keep, new_north * keep


def kernel(
    groups,
    bands,
    sketch_hbm,
    test_hbm,
    stored_hbm,
    chosen,
    row_hbm,
    column_hbm,
    value_hbm,
    increment,
    adjoint,
    total_cost,
    sketch,
    test,
    beyond,
    stored,
    station_row,
    station_column,
    station_value,
    coef_ext,
    ext,
    forced,
    forced_beyond,
    folded,
    spread,
    base_send,
    base_recv,
    field_send,
    field_recv,
    last_send,
    last_recv,
    message,
    later_in,
    own_in,
    cost_out,
    cost_in,
    cost_group_out,
    cost_group_in,
    load_sem,
    beyond_ss,
    beyond_rs,
    base_ss,
    base_rs,
    field_ss,
    field_rs,
    last_ss,
    last_rs,
    later_ss,
    later_rs,
    own_ss,
    own_rs,
    cost_ss,
    cost_rs,
    cost_group_ss,
    cost_group_rs,
):
    rank, fields, rows, columns = sketch.shape
    halo = STEPS
    group = lax.axis_index("tm")
    band = lax.axis_index("lat")
    total_rows = rows * bands
    observed = station_row.shape[1] * bands
    tiles = columns // LANES

    loads = [
        pltpu.make_async_copy(source, target, load_sem.at[index])
        for index, (source, target) in enumerate(
            (
                (row_hbm, station_row),
                (column_hbm, station_column),
                (value_hbm, station_value),
                (stored_hbm, stored),
                (sketch_hbm, sketch),
                (test_hbm, test),
            )
        )
    ]
    for load in loads:
        load.start()

    barrier = pltpu.get_barrier_semaphore()
    devices = groups * bands
    me = group * bands + band

    def greet(offset, carry):
        other = lax.rem(me + offset, devices)
        pl.semaphore_signal(
            barrier,
            inc=1,
            device_id={"tm": other // bands, "lat": lax.rem(other, bands)},
            device_id_type=MESH,
        )
        return carry

    lax.fori_loop(1, devices, greet, 0)

    def remote(source, target, send_sem, recv_sem, where):
        return pltpu.make_async_remote_copy(
            src_ref=source,
            dst_ref=target,
            send_sem=send_sem,
            recv_sem=recv_sem,
            device_id=where,
            device_id_type=MESH,
        )

    below = {"lat": jnp.maximum(band - 1, 0)}
    above = {"lat": jnp.minimum(band + 1, bands - 1)}

    def halo_copies(send, recv, ss, rs, field):
        down = remote(
            send.at[0, field], recv.at[1, field], ss.at[0, field], rs.at[1, field], below
        )
        up = remote(send.at[1, field], recv.at[0, field], ss.at[1, field], rs.at[0, field], above)
        return down, up

    def halo_start(exchange, field):
        recv = exchange[1]
        down, up = halo_copies(*exchange, field)

        @pl.when(band > 0)
        def _():
            down.start()

        @pl.when(band == 0)
        def _():
            recv[0, field] = jnp.zeros(recv.shape[2:], recv.dtype)

        @pl.when(band < bands - 1)
        def _():
            up.start()

        @pl.when(band == bands - 1)
        def _():
            recv[1, field] = jnp.zeros(recv.shape[2:], recv.dtype)

    def halo_wait(exchange):
        @pl.when(band > 0)
        def _():
            for field in range(fields):
                halo_copies(*exchange, field)[1].wait_recv()

        @pl.when(band < bands - 1)
        def _():
            for field in range(fields):
                halo_copies(*exchange, field)[0].wait_recv()

    def halo_drain(exchange):
        @pl.when(band > 0)
        def _():
            for field in range(fields):
                halo_copies(*exchange, field)[0].wait_send()

        @pl.when(band < bands - 1)
        def _():
            for field in range(fields):
                halo_copies(*exchange, field)[1].wait_send()

    base_halo = (base_send, base_recv, base_ss, base_rs)
    field_halo = (field_send, field_recv, field_ss, field_rs)
    last_halo = (last_send, last_recv, last_ss, last_rs)

    for load in loads[:4]:
        load.wait()

    base_half = stored[chosen[0]]
    base = base_half.astype(jnp.float32)
    base_send[0] = base[:, :halo]
    base_send[1] = base[:, rows - halo :]

    cells = lax.broadcasted_iota(jnp.int32, (columns, station_column.shape[1]), 0)
    at_column = cells == station_column[...]
    local_row = station_row[...] - band * rows
    at_row = (
        lax.broadcasted_iota(jnp.int32, (rows, station_row.shape[1]), 0) == local_row
    )
    one_hot = at_column.astype(jnp.float32)
    by_row = jnp.dot(
        base_half[0],
        one_hot.astype(jnp.bfloat16),
        preferred_element_type=jnp.float32,
    )
    seen = jnp.sum(jnp.where(at_row, by_row, 0.0), axis=0, keepdims=True)
    innovation = seen - station_value[...]
    weight = 1.0 + 2.0 * station_row[...].astype(jnp.float32) / total_rows
    weighted = weight * innovation
    cost = jnp.sum(weighted * innovation, axis=1, keepdims=True) / (2.0 * groups * observed)
    cost_row = jnp.broadcast_to(cost, (1, LANES))
    cost_out[...] = cost_row
    source = jnp.where(at_row, weighted / (2.0 * math.sqrt(observed)), 0.0)
    forced[0] = lax.dot_general(
        source,
        one_hot,
        (((1,), (1,)), ((), ())),
        precision=lax.Precision.HIGHEST,
        preferred_element_type=jnp.float32,
    )
    for field in range(1, fields):
        forced[field] = jnp.zeros((rows, columns), jnp.float32)

    eye = lax.broadcasted_iota(jnp.int32, (rank, LANES), 0) == lax.broadcasted_iota(
        jnp.int32, (rank, LANES), 1
    )

    def spread_row(row):
        column = jnp.sum(jnp.where(eye, row, 0.0), axis=1, keepdims=True)
        spread[...] = jnp.broadcast_to(column, (rank, LANES))

    block = 8

    def combined(basis, field):
        def some(index, total):
            for inner in range(block):
                k = index * block + inner
                factor = jnp.broadcast_to(spread[pl.ds(k, 1), :], (rows, LANES))
                total = total + basis[k, field].astype(jnp.float32) * jnp.concatenate(
                    [factor] * tiles, axis=1
                )
            return total

        return lax.fori_loop(0, rank // block, some, jnp.zeros((rows, columns), jnp.float32))

    def fold(pairs):
        def some(index, carry):
            for inner in range(block):
                k = index * block + inner
                product = None
                for basis, values in pairs:
                    for field in range(fields):
                        term = basis[k, field].astype(jnp.float32) * values[field]
                        product = term if product is None else product + term
                total = product[:, :LANES]
                for tile in range(1, tiles):
                    total = total + product[:, tile * LANES : (tile + 1) * LANES]
                folded[k] = total
            return carry

        lax.fori_loop(0, rank // block, some, 0)
        share = jnp.sum(jnp.sum(folded[...], axis=1), axis=1, keepdims=True)
        message[...] = jnp.sum(jnp.where(eye, share, 0.0), axis=0, keepdims=True)

    last_group = groups - 1
    loads[4].wait()

    @pl.when(group == last_group)
    def _():
        fold(((sketch, forced),))

    pl.semaphore_wait(barrier, devices - 1)

    for field in range(fields):
        halo_start(base_halo, field)

    def each(count, first, action):
        for index in range(first, count):
            action(index)

    def later_copy(offset):
        other = lax.rem(band + offset, bands)
        return remote(
            message,
            later_in.at[band],
            later_ss.at[offset],
            later_rs.at[band],
            {"tm": jnp.maximum(group - 1, 0), "lat": other},
        )

    def own_copy(offset):
        other = lax.rem(band + offset, bands)
        return remote(
            message, own_in.at[band], own_ss.at[offset], own_rs.at[band], {"lat": other}
        )

    def own_arrival(offset):
        other = lax.rem(band + offset, bands)
        return remote(
            message, own_in.at[other], own_ss.at[offset], own_rs.at[other], {"lat": other}
        )

    def announce():
        @pl.when(group > 0)
        def _():
            each(bands, 0, lambda offset: later_copy(offset).start())

        each(bands, 1, lambda offset: own_copy(offset).start())
        own_in[band] = message[...]

    @pl.when(group == last_group)
    def _():
        announce()

    def cost_copy(offset):
        other = lax.rem(band + offset, bands)
        return remote(
            cost_out, cost_in.at[band], cost_ss.at[offset], cost_rs.at[band], {"lat": other}
        )

    def cost_arrival(offset):
        other = lax.rem(band + offset, bands)
        return remote(
            cost_out, cost_in.at[other], cost_ss.at[offset], cost_rs.at[other], {"lat": other}
        )

    each(bands, 1, lambda offset: cost_copy(offset).start())
    cost_in[band] = cost_row

    low, high = pl.ds(0, halo), pl.ds(halo, halo)
    top = pl.ds(rows - halo, halo)
    beyond_down = remote(
        sketch.at[:, :, low], beyond.at[:, :, high], beyond_ss.at[0], beyond_rs.at[1], below
    )
    beyond_up = remote(
        sketch.at[:, :, top], beyond.at[:, :, low], beyond_ss.at[1], beyond_rs.at[0], above
    )

    def clear(place):
        def one(k, carry):
            for field in range(fields):
                beyond[k, field, place] = jnp.zeros((halo, columns), beyond.dtype)
            return carry

        lax.fori_loop(0, rank, one, 0)

    @pl.when(group == 0)
    def _():
        @pl.when(band > 0)
        def _():
            beyond_down.start()

        @pl.when(band == 0)
        def _():
            clear(low)

        @pl.when(band < bands - 1)
        def _():
            beyond_up.start()

        @pl.when(band == bands - 1)
        def _():
            clear(high)

    halo_wait(base_halo)
    scales = (0.5 * wave_coef * 0.25, 0.5 * flow_coef * 0.4, 0.5 * flow_coef * 0.4)
    starts = (0.5 * wave_coef, 0.0, 0.0)
    for field in range(fields):
        for place, part in (
            (pl.ds(0, halo), base_recv[0, field]),
            (pl.ds(halo, rows), base[field]),
            (pl.ds(halo + rows, halo), base_recv[1, field]),
        ):
            coef_ext[field, place] = starts[field] + scales[field] * part
    span = rows + 2 * halo
    inside = pl.ds(halo, rows)
    before, after = pl.ds(0, halo), pl.ds(halo + rows, halo)

    def coefs():
        where = band * rows - halo + lax.broadcasted_iota(jnp.int32, (span, columns), 0)
        latitude = where.astype(jnp.float32)
        turn = wave_coef * coriolis_coef * (2.0 * (latitude + 0.5) / total_rows - 1.0)
        keep = jnp.where((where >= 0) & (where < total_rows), 1.0, 0.0)
        return coef_ext[0], coef_ext[1], coef_ext[2], turn, keep

    def march(step_of):
        def one(index, carry):
            result = step_of((ext[0], ext[1], ext[2]), coefs())
            for field in range(fields):
                ext[field] = result[field]
            return carry

        lax.fori_loop(0, STEPS, one, 0)

    def banded(basis, exchange):
        send, recv = exchange[:2]
        for field in range(fields):
            total = combined(basis, field)
            send[0, field] = total[:halo]
            send[1, field] = total[rows - halo :]
            halo_start(exchange, field)
            ext[field, inside] = total
        halo_wait(exchange)
        for field in range(fields):
            ext[field, before] = recv[0, field]
            ext[field, after] = recv[1, field]

    map_factor = map_scale / math.sqrt(rank * fields * total_rows * columns)

    def add_mapped():
        for field in range(fields):
            forced[field] = forced[field] + map_factor * ext[field, inside]

    loads[5].wait()

    @pl.when(group < last_group)
    def _():
        def arrive(offset):
            remote(
                message,
                later_in.at[offset],
                later_ss.at[offset],
                later_rs.at[offset],
                {"tm": group, "lat": offset},
            ).wait_recv()

        each(bands, 0, arrive)
        spread_row(jnp.sum(later_in[...], axis=0))

        @pl.when(group > 0)
        def _():
            banded(test, field_halo)
            march(advance_adjoint)
            add_mapped()
            fold(((sketch, forced),))

        @pl.when(group == 0)
        def _():
            for field in range(fields):
                ext[field, inside] = combined(test, field)
                ext[field, before] = jnp.zeros((halo, columns), jnp.float32)
                ext[field, after] = jnp.zeros((halo, columns), jnp.float32)
            march(advance_adjoint)
            add_mapped()
            for field in range(fields):
                forced_beyond[field, low] = map_factor * ext[field, before]
                forced_beyond[field, high] = map_factor * ext[field, after]

            @pl.when(band > 0)
            def _():
                beyond_up.wait_recv()

            @pl.when(band < bands - 1)
            def _():
                beyond_down.wait_recv()

            fold(((sketch, forced), (beyond, forced_beyond)))

        announce()

    each(bands, 1, lambda offset: cost_arrival(offset).wait_recv())
    group_cost = jnp.sum(cost_in[...], axis=0)
    cost_group_out[...] = group_cost

    def cost_group_copy(offset):
        other = lax.rem(group + offset, groups)
        return remote(
            cost_group_out,
            cost_group_in.at[group],
            cost_group_ss.at[offset],
            cost_group_rs.at[group],
            {"tm": other},
        )

    def cost_group_arrival(offset):
        other = lax.rem(group + offset, groups)
        return remote(
            cost_group_out,
            cost_group_in.at[other],
            cost_group_ss.at[offset],
            cost_group_rs.at[other],
            {"tm": other},
        )

    each(groups, 1, lambda offset: cost_group_copy(offset).start())
    cost_group_in[group] = group_cost

    each(bands, 1, lambda offset: own_arrival(offset).wait_recv())
    adjoint_row = jnp.sum(own_in[...], axis=0)
    adjoint[...] = adjoint_row[:, :rank]
    spread_row(adjoint_row)

    @pl.when(group > 0)
    def _():
        banded(sketch, last_halo)

    @pl.when(group == 0)
    def _():
        for field in range(fields):
            ext[field, inside] = combined(sketch, field)
            outer = combined(beyond, field)
            ext[field, before] = outer[:halo]
            ext[field, after] = outer[halo:]

    march(advance)
    for field in range(fields):
        increment[0, field] = ext[field, inside] / math.sqrt(rank)

    each(groups, 1, lambda offset: cost_group_arrival(offset).wait_recv())
    total_cost[...] = jnp.sum(cost_group_in[...], axis=0)[:, :1]

    halo_drain(base_halo)
    each(bands, 1, lambda offset: cost_copy(offset).wait_send())
    each(bands, 1, lambda offset: own_copy(offset).wait_send())
    each(groups, 1, lambda offset: cost_group_copy(offset).wait_send())

    @pl.when(group > 0)
    def _():
        halo_drain(last_halo)
        each(bands, 0, lambda offset: later_copy(offset).wait_send())

    @pl.when((group > 0) & (group < last_group))
    def _():
        halo_drain(field_halo)

    @pl.when(group == 0)
    def _():
        @pl.when(band > 0)
        def _():
            beyond_down.wait_send()

        @pl.when(band < bands - 1)
        def _():
            beyond_up.wait_send()


def body(
    groups,
    bands,
    sketch,
    test_sketch,
    checkpoints,
    checkpoint_step,
    station_row,
    station_column,
    station_value,
):
    rank, fields, rows, columns = sketch.shape
    span = rows + 2 * STEPS
    f32 = jnp.float32
    vmem = pl.BlockSpec(memory_space=pltpu.VMEM)
    hbm = pl.BlockSpec(memory_space=pltpu.HBM)
    edge = pltpu.VMEM((2, fields, STEPS, columns), f32)
    dma = pltpu.SemaphoreType.DMA
    increment, adjoint, cost = pl.pallas_call(
        functools.partial(kernel, groups, bands),
        out_shape=(
            jax.ShapeDtypeStruct((1, fields, rows, columns), f32),
            jax.ShapeDtypeStruct((1, rank), f32),
            jax.ShapeDtypeStruct((1, 1), f32),
        ),
        in_specs=[hbm, hbm, hbm, pl.BlockSpec(memory_space=pltpu.SMEM), hbm, hbm, hbm],
        out_specs=(vmem, vmem, vmem),
        scratch_shapes=[
            pltpu.VMEM(sketch.shape, sketch.dtype),
            pltpu.VMEM(test_sketch.shape, test_sketch.dtype),
            pltpu.VMEM((rank, fields, 2 * STEPS, columns), sketch.dtype),
            pltpu.VMEM(checkpoints.shape, checkpoints.dtype),
            pltpu.VMEM(station_row.shape, station_row.dtype),
            pltpu.VMEM(station_column.shape, station_column.dtype),
            pltpu.VMEM(station_value.shape, station_value.dtype),
            pltpu.VMEM((fields, span, columns), f32),
            pltpu.VMEM((fields, span, columns), f32),
            pltpu.VMEM((fields, rows, columns), f32),
            pltpu.VMEM((fields, 2 * STEPS, columns), f32),
            pltpu.VMEM((rank, rows, LANES), f32),
            pltpu.VMEM((rank, LANES), f32),
            edge,
            edge,
            edge,
            edge,
            edge,
            edge,
            pltpu.VMEM((1, LANES), f32),
            pltpu.VMEM((bands, 1, LANES), f32),
            pltpu.VMEM((bands, 1, LANES), f32),
            pltpu.VMEM((1, LANES), f32),
            pltpu.VMEM((bands, 1, LANES), f32),
            pltpu.VMEM((1, LANES), f32),
            pltpu.VMEM((groups, 1, LANES), f32),
            dma((6,)),
            dma((2,)),
            dma((2,)),
            dma((2, fields)),
            dma((2, fields)),
            dma((2, fields)),
            dma((2, fields)),
            dma((2, fields)),
            dma((2, fields)),
            dma((bands,)),
            dma((bands,)),
            dma((bands,)),
            dma((bands,)),
            dma((bands,)),
            dma((bands,)),
            dma((groups,)),
            dma((groups,)),
        ],
        compiler_params=pltpu.CompilerParams(
            collective_id=0,
            has_side_effects=True,
            vmem_limit_bytes=67043328,
        ),
    )(
        sketch,
        test_sketch,
        checkpoints,
        checkpoint_step,
        station_row,
        station_column,
        station_value,
    )
    return increment, adjoint, cost[0, 0]


def solution(mesh):
    placed = (
        P("tm", None, "lat", None),
        P("tm", None, "lat", None),
        P("tm", None, "lat", None),
        P("tm"),
        P("tm", "lat"),
        P("tm", "lat"),
        P("tm", "lat"),
    )
    return jax.shard_map(
        functools.partial(body, mesh.shape["tm"], mesh.shape["lat"]),
        mesh=mesh,
        in_specs=placed,
        out_specs=(P("tm", None, "lat", None), P("tm", None), P()),
        check_vma=False,
    )
```

```python
import functools
import math

import jax
import jax.numpy as jnp
from jax import lax
from jax.experimental import pallas as pl
from jax.experimental.pallas import tpu as pltpu
from jax.sharding import PartitionSpec as P

STEPS = 4
LANES = 128

wave_coef = 0.5
flow_coef = 0.4
coriolis_coef = 0.5
map_scale = 0.5

MESH = pl.DeviceIdType.MESH


def dlon(field):
    count = field.shape[1]
    return pltpu.roll(field, count - 1, 1) - pltpu.roll(field, 1, 1)


def dlat(field):
    count = field.shape[0]
    return pltpu.roll(field, count - 1, 0) - pltpu.roll(field, 1, 0)


def advance(state, coefs):
    height, east, north = state
    depth, east_flow, north_flow, turn, keep = coefs
    half = 0.5 * wave_coef
    dx_east, dy_north = dlon(east), dlat(north)
    dx_height, dy_height = dlon(height), dlat(height)
    new_east = (
        east + turn * north - half * dx_height - (east_flow * dx_east + north_flow * dlat(east))
    )
    new_north = (
        north - turn * east - half * dy_height - (east_flow * dlon(north) + north_flow * dy_north)
    )
    new_height = (
        height - depth * (dx_east + dy_north) - (east_flow * dx_height + north_flow * dy_height)
    )
    return new_height * keep, new_east * keep, new_north * keep


def advance_adjoint(state, coefs):
    height, east, north = state
    depth, east_flow, north_flow, turn, keep = coefs
    half = 0.5 * wave_coef
    deep = depth * height
    new_height = height + dlon(half * east + east_flow * height) + dlat(
        half * north + north_flow * height
    )
    new_east = east - turn * north + dlon(deep + east_flow * east) + dlat(north_flow * east)
    new_north = north + turn * east + dlon(east_flow * north) + dlat(deep + north_flow * north)
    return new_height * keep, new_east * keep, new_north * keep


def kernel(
    groups,
    bands,
    sketch_hbm,
    test_hbm,
    stored_hbm,
    chosen,
    row_hbm,
    column_hbm,
    value_hbm,
    increment,
    adjoint,
    total_cost,
    sketch,
    test,
    beyond,
    stored,
    station_row,
    station_column,
    station_value,
    coef_ext,
    ext,
    forced,
    forced_beyond,
    folded,
    spread,
    base_send,
    base_recv,
    field_send,
    field_recv,
    last_send,
    last_recv,
    message,
    later_in,
    own_in,
    cost_out,
    cost_in,
    cost_group_out,
    cost_group_in,
    load_sem,
    beyond_ss,
    beyond_rs,
    base_ss,
    base_rs,
    field_ss,
    field_rs,
    last_ss,
    last_rs,
    later_ss,
    later_rs,
    own_ss,
    own_rs,
    cost_ss,
    cost_rs,
    cost_group_ss,
    cost_group_rs,
):
    rank, fields, rows, columns = sketch.shape
    halo = STEPS
    group = lax.axis_index("tm")
    band = lax.axis_index("lat")
    total_rows = rows * bands
    observed = station_row.shape[1] * bands
    tiles = columns // LANES

    loads = [
        pltpu.make_async_copy(source, target, load_sem.at[index])
        for index, (source, target) in enumerate(
            (
                (row_hbm, station_row),
                (column_hbm, station_column),
                (value_hbm, station_value),
                (stored_hbm, stored),
                (sketch_hbm, sketch),
                (test_hbm, test),
            )
        )
    ]
    for load in loads[:5]:
        load.start()

    barrier = pltpu.get_barrier_semaphore()
    last_group = groups - 1

    def each(count, first, action):
        for index in range(first, count):
            action(index)

    def greet(place):
        pl.semaphore_signal(barrier, inc=1, device_id=place, device_id_type=MESH)

    @pl.when(group < last_group)
    def _():
        each(bands, 0, lambda index: greet({"tm": group + 1, "lat": index}))

    @pl.when(group > 0)
    def _():
        each(bands, 0, lambda index: greet({"tm": group - 1, "lat": index}))

    each(bands, 1, lambda offset: greet({"lat": lax.rem(band + offset, bands)}))

    for offset in range(2, groups):

        @pl.when(group + offset < groups)
        def _():
            greet({"tm": group + offset})

        @pl.when(group - offset >= 0)
        def _():
            greet({"tm": group - offset})

    sides = jnp.minimum(group, 1) + jnp.minimum(last_group - group, 1)
    greetings = bands - 1 + bands * sides + groups - 1 - sides

    def remote(source, target, send_sem, recv_sem, where):
        return pltpu.make_async_remote_copy(
            src_ref=source,
            dst_ref=target,
            send_sem=send_sem,
            recv_sem=recv_sem,
            device_id=where,
            device_id_type=MESH,
        )

    below = {"lat": jnp.maximum(band - 1, 0)}
    above = {"lat": jnp.minimum(band + 1, bands - 1)}

    def halo_copies(send, recv, ss, rs, field):
        down = remote(
            send.at[0, field], recv.at[1, field], ss.at[0, field], rs.at[1, field], below
        )
        up = remote(send.at[1, field], recv.at[0, field], ss.at[1, field], rs.at[0, field], above)
        return down, up

    def halo_start(exchange, field):
        recv = exchange[1]
        down, up = halo_copies(*exchange, field)

        @pl.when(band > 0)
        def _():
            down.start()

        @pl.when(band == 0)
        def _():
            recv[0, field] = jnp.zeros(recv.shape[2:], recv.dtype)

        @pl.when(band < bands - 1)
        def _():
            up.start()

        @pl.when(band == bands - 1)
        def _():
            recv[1, field] = jnp.zeros(recv.shape[2:], recv.dtype)

    def halo_wait(exchange):
        @pl.when(band > 0)
        def _():
            for field in range(fields):
                halo_copies(*exchange, field)[1].wait_recv()

        @pl.when(band < bands - 1)
        def _():
            for field in range(fields):
                halo_copies(*exchange, field)[0].wait_recv()

    def halo_drain(exchange):
        @pl.when(band > 0)
        def _():
            for field in range(fields):
                halo_copies(*exchange, field)[0].wait_send()

        @pl.when(band < bands - 1)
        def _():
            for field in range(fields):
                halo_copies(*exchange, field)[1].wait_send()

    base_halo = (base_send, base_recv, base_ss, base_rs)
    field_halo = (field_send, field_recv, field_ss, field_rs)
    last_halo = (last_send, last_recv, last_ss, last_rs)

    for load in loads[:4]:
        load.wait()

    base_half = stored[chosen[0]]
    base = base_half.astype(jnp.float32)
    base_send[0] = base[:, :halo]
    base_send[1] = base[:, rows - halo :]

    cells = lax.broadcasted_iota(jnp.int32, (columns, station_column.shape[1]), 0)
    at_column = cells == station_column[...]
    local_row = station_row[...] - band * rows
    at_row = (
        lax.broadcasted_iota(jnp.int32, (rows, station_row.shape[1]), 0) == local_row
    )
    one_hot = at_column.astype(jnp.float32)
    by_row = jnp.dot(
        base_half[0],
        one_hot.astype(jnp.bfloat16),
        preferred_element_type=jnp.float32,
    )
    seen = jnp.sum(jnp.where(at_row, by_row, 0.0), axis=0, keepdims=True)
    innovation = seen - station_value[...]
    weight = 1.0 + 2.0 * station_row[...].astype(jnp.float32) / total_rows
    weighted = weight * innovation
    cost = jnp.sum(weighted * innovation, axis=1, keepdims=True) / (2.0 * groups * observed)
    cost_row = jnp.broadcast_to(cost, (1, LANES))
    cost_out[...] = cost_row
    source = jnp.where(at_row, weighted / (2.0 * math.sqrt(observed)), 0.0)
    forced[0] = lax.dot_general(
        source,
        one_hot,
        (((1,), (1,)), ((), ())),
        precision=lax.Precision.HIGHEST,
        preferred_element_type=jnp.float32,
    )
    for field in range(1, fields):
        forced[field] = jnp.zeros((rows, columns), jnp.float32)

    eye = lax.broadcasted_iota(jnp.int32, (rank, LANES), 0) == lax.broadcasted_iota(
        jnp.int32, (rank, LANES), 1
    )

    def spread_row(row):
        column = jnp.sum(jnp.where(eye, row, 0.0), axis=1, keepdims=True)
        spread[...] = jnp.broadcast_to(column, (rank, LANES))

    block = 8

    def combined(basis, field):
        def some(index, total):
            for inner in range(block):
                k = index * block + inner
                factor = jnp.broadcast_to(spread[pl.ds(k, 1), :], (rows, LANES))
                total = total + basis[k, field].astype(jnp.float32) * jnp.concatenate(
                    [factor] * tiles, axis=1
                )
            return total

        return lax.fori_loop(0, rank // block, some, jnp.zeros((rows, columns), jnp.float32))

    def fold(pairs):
        def some(index, carry):
            for inner in range(block):
                k = index * block + inner
                product = None
                for basis, values in pairs:
                    for field in range(fields):
                        term = basis[k, field].astype(jnp.float32) * values[field]
                        product = term if product is None else product + term
                total = product[:, :LANES]
                for tile in range(1, tiles):
                    total = total + product[:, tile * LANES : (tile + 1) * LANES]
                folded[k] = total
            return carry

        lax.fori_loop(0, rank // block, some, 0)
        share = jnp.sum(jnp.sum(folded[...], axis=1), axis=1, keepdims=True)
        message[...] = jnp.sum(jnp.where(eye, share, 0.0), axis=0, keepdims=True)

    loads[4].wait()

    @pl.when(group < last_group)
    def _():
        loads[5].start()

    @pl.when(group == last_group)
    def _():
        fold(((sketch, forced),))

    pl.semaphore_wait(barrier, greetings)

    def later_copy(offset):
        other = lax.rem(band + offset, bands)
        return remote(
            message,
            later_in.at[band],
            later_ss.at[offset],
            later_rs.at[band],
            {"tm": jnp.maximum(group - 1, 0), "lat": other},
        )

    def own_copy(offset):
        other = lax.rem(band + offset, bands)
        return remote(
            message, own_in.at[band], own_ss.at[offset], own_rs.at[band], {"lat": other}
        )

    def own_arrival(offset):
        other = lax.rem(band + offset, bands)
        return remote(
            message, own_in.at[other], own_ss.at[offset], own_rs.at[other], {"lat": other}
        )

    def announce():
        @pl.when(group > 0)
        def _():
            each(bands, 0, lambda offset: later_copy(offset).start())

        each(bands, 1, lambda offset: own_copy(offset).start())
        own_in[band] = message[...]

    @pl.when(group == last_group)
    def _():
        announce()

    for field in range(fields):
        halo_start(base_halo, field)

    def cost_copy(offset):
        other = lax.rem(band + offset, bands)
        return remote(
            cost_out, cost_in.at[band], cost_ss.at[offset], cost_rs.at[band], {"lat": other}
        )

    def cost_arrival(offset):
        other = lax.rem(band + offset, bands)
        return remote(
            cost_out, cost_in.at[other], cost_ss.at[offset], cost_rs.at[other], {"lat": other}
        )

    each(bands, 1, lambda offset: cost_copy(offset).start())
    cost_in[band] = cost_row

    low, high = pl.ds(0, halo), pl.ds(halo, halo)
    top = pl.ds(rows - halo, halo)
    beyond_down = remote(
        sketch.at[:, :, low], beyond.at[:, :, high], beyond_ss.at[0], beyond_rs.at[1], below
    )
    beyond_up = remote(
        sketch.at[:, :, top], beyond.at[:, :, low], beyond_ss.at[1], beyond_rs.at[0], above
    )

    def clear(place):
        def one(k, carry):
            for field in range(fields):
                beyond[k, field, place] = jnp.zeros((halo, columns), beyond.dtype)
            return carry

        lax.fori_loop(0, rank, one, 0)

    @pl.when(group == 0)
    def _():
        @pl.when(band > 0)
        def _():
            beyond_down.start()

        @pl.when(band == 0)
        def _():
            clear(low)

        @pl.when(band < bands - 1)
        def _():
            beyond_up.start()

        @pl.when(band == bands - 1)
        def _():
            clear(high)

    halo_wait(base_halo)
    scales = (0.5 * wave_coef * 0.25, 0.5 * flow_coef * 0.4, 0.5 * flow_coef * 0.4)
    starts = (0.5 * wave_coef, 0.0, 0.0)
    for field in range(fields):
        for place, part in (
            (pl.ds(0, halo), base_recv[0, field]),
            (pl.ds(halo, rows), base[field]),
            (pl.ds(halo + rows, halo), base_recv[1, field]),
        ):
            coef_ext[field, place] = starts[field] + scales[field] * part
    span = rows + 2 * halo
    inside = pl.ds(halo, rows)
    before, after = pl.ds(0, halo), pl.ds(halo + rows, halo)

    def coefs():
        where = band * rows - halo + lax.broadcasted_iota(jnp.int32, (span, columns), 0)
        latitude = where.astype(jnp.float32)
        turn = wave_coef * coriolis_coef * (2.0 * (latitude + 0.5) / total_rows - 1.0)
        keep = jnp.where((where >= 0) & (where < total_rows), 1.0, 0.0)
        return coef_ext[0], coef_ext[1], coef_ext[2], turn, keep

    def march(step_of):
        def one(index, carry):
            result = step_of((ext[0], ext[1], ext[2]), coefs())
            for field in range(fields):
                ext[field] = result[field]
            return carry

        lax.fori_loop(0, STEPS, one, 0)

    def banded(basis, exchange):
        send, recv = exchange[:2]
        for field in range(fields):
            total = combined(basis, field)
            send[0, field] = total[:halo]
            send[1, field] = total[rows - halo :]
            halo_start(exchange, field)
            ext[field, inside] = total
        halo_wait(exchange)
        for field in range(fields):
            ext[field, before] = recv[0, field]
            ext[field, after] = recv[1, field]

    map_factor = map_scale / math.sqrt(rank * fields * total_rows * columns)

    def add_mapped():
        for field in range(fields):
            forced[field] = forced[field] + map_factor * ext[field, inside]

    @pl.when(group < last_group)
    def _():
        def arrive(offset):
            remote(
                message,
                later_in.at[offset],
                later_ss.at[offset],
                later_rs.at[offset],
                {"tm": group, "lat": offset},
            ).wait_recv()

        loads[5].wait()
        each(bands, 0, arrive)
        spread_row(jnp.sum(later_in[...], axis=0))

        @pl.when(group > 0)
        def _():
            banded(test, field_halo)
            march(advance_adjoint)
            add_mapped()
            fold(((sketch, forced),))

        @pl.when(group == 0)
        def _():
            for field in range(fields):
                ext[field, inside] = combined(test, field)
                ext[field, before] = jnp.zeros((halo, columns), jnp.float32)
                ext[field, after] = jnp.zeros((halo, columns), jnp.float32)
            march(advance_adjoint)
            add_mapped()
            for field in range(fields):
                forced_beyond[field, low] = map_factor * ext[field, before]
                forced_beyond[field, high] = map_factor * ext[field, after]

            @pl.when(band > 0)
            def _():
                beyond_up.wait_recv()

            @pl.when(band < bands - 1)
            def _():
                beyond_down.wait_recv()

            fold(((sketch, forced), (beyond, forced_beyond)))

        announce()

    each(bands, 1, lambda offset: cost_arrival(offset).wait_recv())
    group_cost = jnp.sum(cost_in[...], axis=0)
    cost_group_out[...] = group_cost

    def cost_group_copy(offset):
        other = lax.rem(group + offset, groups)
        return remote(
            cost_group_out,
            cost_group_in.at[group],
            cost_group_ss.at[offset],
            cost_group_rs.at[group],
            {"tm": other},
        )

    def cost_group_arrival(offset):
        other = lax.rem(group + offset, groups)
        return remote(
            cost_group_out,
            cost_group_in.at[other],
            cost_group_ss.at[offset],
            cost_group_rs.at[other],
            {"tm": other},
        )

    each(groups, 1, lambda offset: cost_group_copy(offset).start())
    cost_group_in[group] = group_cost

    each(bands, 1, lambda offset: own_arrival(offset).wait_recv())
    adjoint_row = jnp.sum(own_in[...], axis=0)
    adjoint[...] = adjoint_row[:, :rank]
    spread_row(adjoint_row)

    @pl.when(group > 0)
    def _():
        banded(sketch, last_halo)

    @pl.when(group == 0)
    def _():
        for field in range(fields):
            ext[field, inside] = combined(sketch, field)
            outer = combined(beyond, field)
            ext[field, before] = outer[:halo]
            ext[field, after] = outer[halo:]

    march(advance)
    for field in range(fields):
        increment[0, field] = ext[field, inside] / math.sqrt(rank)

    each(groups, 1, lambda offset: cost_group_arrival(offset).wait_recv())
    total_cost[...] = jnp.sum(cost_group_in[...], axis=0)[:, :1]

    halo_drain(base_halo)
    each(bands, 1, lambda offset: cost_copy(offset).wait_send())
    each(bands, 1, lambda offset: own_copy(offset).wait_send())
    each(groups, 1, lambda offset: cost_group_copy(offset).wait_send())

    @pl.when(group > 0)
    def _():
        halo_drain(last_halo)
        each(bands, 0, lambda offset: later_copy(offset).wait_send())

    @pl.when((group > 0) & (group < last_group))
    def _():
        halo_drain(field_halo)

    @pl.when(group == 0)
    def _():
        @pl.when(band > 0)
        def _():
            beyond_down.wait_send()

        @pl.when(band < bands - 1)
        def _():
            beyond_up.wait_send()


def body(
    groups,
    bands,
    sketch,
    test_sketch,
    checkpoints,
    checkpoint_step,
    station_row,
    station_column,
    station_value,
):
    rank, fields, rows, columns = sketch.shape
    span = rows + 2 * STEPS
    f32 = jnp.float32

    def in_hbm(array):
        return pltpu.with_memory_space_constraint(array, pltpu.HBM)

    vmem = pl.BlockSpec(memory_space=pltpu.VMEM)
    hbm = pl.BlockSpec(memory_space=pltpu.HBM)
    edge = pltpu.VMEM((2, fields, STEPS, columns), f32)
    dma = pltpu.SemaphoreType.DMA
    increment, adjoint, cost = pl.pallas_call(
        functools.partial(kernel, groups, bands),
        out_shape=(
            jax.ShapeDtypeStruct((1, fields, rows, columns), f32),
            jax.ShapeDtypeStruct((1, rank), f32),
            jax.ShapeDtypeStruct((1, 1), f32),
        ),
        in_specs=[hbm, hbm, hbm, pl.BlockSpec(memory_space=pltpu.SMEM), hbm, hbm, hbm],
        out_specs=(vmem, vmem, vmem),
        scratch_shapes=[
            pltpu.VMEM(sketch.shape, sketch.dtype),
            pltpu.VMEM(test_sketch.shape, test_sketch.dtype),
            pltpu.VMEM((rank, fields, 2 * STEPS, columns), sketch.dtype),
            pltpu.VMEM(checkpoints.shape, checkpoints.dtype),
            pltpu.VMEM(station_row.shape, station_row.dtype),
            pltpu.VMEM(station_column.shape, station_column.dtype),
            pltpu.VMEM(station_value.shape, station_value.dtype),
            pltpu.VMEM((fields, span, columns), f32),
            pltpu.VMEM((fields, span, columns), f32),
            pltpu.VMEM((fields, rows, columns), f32),
            pltpu.VMEM((fields, 2 * STEPS, columns), f32),
            pltpu.VMEM((rank, rows, LANES), f32),
            pltpu.VMEM((rank, LANES), f32),
            edge,
            edge,
            edge,
            edge,
            edge,
            edge,
            pltpu.VMEM((1, LANES), f32),
            pltpu.VMEM((bands, 1, LANES), f32),
            pltpu.VMEM((bands, 1, LANES), f32),
            pltpu.VMEM((1, LANES), f32),
            pltpu.VMEM((bands, 1, LANES), f32),
            pltpu.VMEM((1, LANES), f32),
            pltpu.VMEM((groups, 1, LANES), f32),
            dma((6,)),
            dma((2,)),
            dma((2,)),
            dma((2, fields)),
            dma((2, fields)),
            dma((2, fields)),
            dma((2, fields)),
            dma((2, fields)),
            dma((2, fields)),
            dma((bands,)),
            dma((bands,)),
            dma((bands,)),
            dma((bands,)),
            dma((bands,)),
            dma((bands,)),
            dma((groups,)),
            dma((groups,)),
        ],
        compiler_params=pltpu.CompilerParams(
            collective_id=0,
            has_side_effects=True,
            vmem_limit_bytes=24 * 1024 * 1024,
        ),
    )(
        in_hbm(sketch),
        in_hbm(test_sketch),
        in_hbm(checkpoints),
        checkpoint_step,
        in_hbm(station_row),
        in_hbm(station_column),
        in_hbm(station_value),
    )
    return increment, adjoint, cost[0, 0]


def solution(mesh):
    placed = (
        P("tm", None, "lat", None),
        P("tm", None, "lat", None),
        P("tm", None, "lat", None),
        P("tm"),
        P("tm", "lat"),
        P("tm", "lat"),
        P("tm", "lat"),
    )
    return jax.shard_map(
        functools.partial(body, mesh.shape["tm"], mesh.shape["lat"]),
        mesh=mesh,
        in_specs=placed,
        out_specs=(P("tm", None, "lat", None), P("tm", None), P()),
        check_vma=False,
    )
```
